256 devices in a mesh: tm: 2 (over z_lo), chan: 32 (over y, x, core), bl: 4 (over z_hi).
Axes of the slice: x: 4, y: 4, z: 8 (z_hi: 4, z_lo: 2; z = z_hi * 2 + z_lo), core: 2. Of those that a mesh axis runs over, the one named last changes fastest.
Arguments:
- voltages: bfloat16 [2, 256, 1024, 512], P(None, ('chan', 'bl'), None, 'tm'), may hold values from -6 to 6
Outputs:
- visibilities: bfloat16 [2, 1024, 4, 256, 256], P(None, ('chan', 'bl'), 'tm')
The draws below stay inside these ranges and needn't reach their ends.
All inputs are finite; a program needn't handle non-finite values.
Results may differ from the reference program's by a relative error of at most 0.0051.
Values may be sent and summed in bfloat16 or wider, within the bound.
A program may use at most 64 MiB of HBM per device.

```python
import jax
import jax.numpy as jnp
from jax import lax

SIG = 256
CH_DEV = 8
CHANNELS = 1024
HALF = 128
TIME = 512
WIN = 4


def block_levels(stream_key, dims, pieces, least, top_value):
    gain, own = 1.0, jax.random.fold_in(stream_key, 6)
    for position, parts in pieces:
        heights = jnp.exp(jax.random.uniform(jax.random.fold_in(own, position), (parts,), jnp.float32, least / len(pieces), top_value / len(pieces)))
        gain = gain * jnp.repeat(heights, dims[position] // parts).reshape([-1 if axis == position else 1 for axis in range(len(dims))])
    return gain


def scatter_about(key, dims, deviation, limit, shards=(), kind=jnp.bfloat16):
    values = jax.random.normal(key, dims, jnp.float32) * deviation
    if len(shards) > 0:
        values = block_levels(key, dims, shards, -0.22, 0.18) * values
    return jnp.clip(values, min=-limit, max=limit).astype(kind)


def setup_inputs(seed: int = 0) -> dict:
    key_list = jax.random.split(jax.random.key(seed), 2)
    voltages = scatter_about(key_list[0], (2, SIG, CHANNELS, TIME), 1.0, 6.0, ((1, 128), (3, 2)))
    return dict(voltages=voltages)


def tapers(length):
    steps = jnp.arange(length, dtype=jnp.float32)
    taper_early = jnp.sin(jnp.pi * (steps + 0.5) / (2.0 * length))
    taper_late = jnp.sin(jnp.pi * (steps + 0.5 + length) / (2.0 * length))
    return taper_early, taper_late


def weighted(block, taper):
    return (block.astype(jnp.float32) * taper).astype(jnp.bfloat16)


def products(stacked):
    signals = stacked.shape[0] // 2
    wide = stacked.astype(jnp.float32)
    gram = jnp.einsum("pct,qct->cpq", wide, wide, precision=lax.Precision.HIGHEST)
    real_part = gram[:, :signals, :signals] + gram[:, signals:, signals:]
    imag_part = gram[:, signals:, :signals] - gram[:, :signals, signals:]
    return real_part, imag_part


def reference(voltages):
    taper_early, taper_late = tapers(HALF)
    groups = CHANNELS // CH_DEV
    halves = TIME // HALF
    scale = 1.0 / HALF

    def one_group(group):
        block = lax.dynamic_slice_in_dim(voltages, group * CH_DEV, CH_DEV, 2)
        stacked = block.reshape(2 * SIG, CH_DEV, TIME)
        previous = (jnp.zeros((CH_DEV, SIG, SIG), jnp.float32), jnp.zeros((CH_DEV, SIG, SIG), jnp.float32))
        real_list = []
        imag_list = []
        for index in range(halves):
            piece = stacked[:, :, index * HALF:(index + 1) * HALF]
            late_real, late_imag = products(weighted(piece, taper_late))
            real_list.append(((late_real + previous[0]) * scale).astype(jnp.bfloat16))
            imag_list.append(((late_imag + previous[1]) * scale).astype(jnp.bfloat16))
            previous = products(weighted(piece, taper_early))
        return jnp.stack([jnp.stack(real_list, 1), jnp.stack(imag_list, 1)], 0)

    result = lax.map(one_group, jnp.arange(groups, dtype=jnp.int32))
    return jnp.transpose(result, (1, 0, 2, 3, 4, 5)).reshape(2, CHANNELS, WIN, SIG, SIG)
```

```python
import jax, jax.numpy as jnp, functools
from jax import lax
from jax.sharding import PartitionSpec as P
from jax.experimental import pallas as pl
from jax.experimental.pallas import tpu as pltpu
MESH = pl.DeviceIdType.MESH
FL = dict(relay=True, order=(3, 1, 2, 0), lag=4, xy=True)

def comm_kernel(fl, v, out, s, g, rxy, rz, sx, sz, sr, fin):
    t, c, b = lax.axis_index("tm"), lax.axis_index("chan"), lax.axis_index("bl")
    y, l = lax.div(c, 8), lax.rem(c, 8)

    def piece(cc, bb, half):
        return v.at[:, :, cc * 4 + bb, :, pl.ds(half * 128, 128)]

    def spot(o, half, cc):
        return g.at[half, b, cc] if o == 0 else s.at[o - 1, half, cc]

    sem = pltpu.get_barrier_semaphore()
    def greet(**k):
        pl.semaphore_signal(sem, inc=1, device_id=k, device_id_type=MESH)
    for o in (2, 1, 3):
        greet(bl=lax.rem(b + o, 4))
    greet(tm=1 - t)
    far = jnp.where(t == 0, 1, -1)
    greet(tm=1 - t, bl=lax.rem(b - 2 * far + 8, 4))
    greet(tm=1 - t, bl=lax.rem(b - far + 8, 4))
    def greet_xy(i, _):
        greet(chan=lax.rem(c + i, 32))
        return 0
    lax.fori_loop(1, 32, greet_xy, 0)
    for half in (1, 0):
        for o in (2, 3, 1, 0):
            pltpu.make_async_copy(piece(c, lax.rem(b + o, 4), half), spot(o, half, c), rxy.at[o, half, y]).start()
    pl.semaphore_wait(sem, 37)
    if not fl["xy"]:
        for half in (1, 0):
            for o in range(4):
                pltpu.make_async_copy(piece(c, lax.rem(b + o, 4), half), spot(o, half, c), rxy.at[o, half, y]).wait()

    def xysend(half, o, d):
        def send(j, _):
            cc = lax.rem(y + d, 4) * 8 + lax.rem(l + j, 8)
            pltpu.make_async_remote_copy(
                src_ref=piece(cc, lax.rem(b + o, 4), half), dst_ref=spot(o, half, c),
                send_sem=sx.at[o, half], recv_sem=rxy.at[o, half, y],
                device_id={"chan": cc}, device_id_type=MESH).start()
            return 0
        lax.fori_loop(1 if d == 0 else 0, 8, send, 0)

    def rows(ref):
        return ref
    def arrived(ref, sm):
        pltpu.make_async_copy(ref, ref, sm).wait()

    def yg(d):
        return lax.rem(y + 4 - d, 4)
    def eight(d):
        return pl.ds(pl.multiple_of(yg(d) * 8, 8), 8)

    def zsend(half, o, d):
        part = s.at[o - 1, half, eight(d)]
        if fl["xy"]: arrived(part, rxy.at[o, half, yg(d)])
        if half == 1 and o != 1 and fl["relay"]:
            to_t = jnp.int32(1)
            h = jnp.where(t == 0, 2, 1)
        else:
            to_t, h = t, half
        pltpu.make_async_remote_copy(
            src_ref=part, dst_ref=g.at[h, b, eight(d)],
            send_sem=sz.at[o, half], recv_sem=rz.at[h, o, yg(d)],
            device_id={"bl": lax.rem(b + o, 4), "tm": to_t}, device_id_type=MESH).start()

    def relay(d, o, h_from, h_to):
        src = lax.rem(b + 4 - o, 4)
        pltpu.make_async_remote_copy(
            src_ref=g.at[h_from, src, eight(d)], dst_ref=g.at[h_to, src, eight(d)],
            send_sem=sr.at[o], recv_sem=rz.at[h_to, o, yg(d)],
            device_id={"tm": 1 - t}, device_id_type=MESH).start()

    def landed(h, o, d):
        arrived(g.at[h, lax.rem(b + 4 - o, 4), eight(d)], rz.at[h, o, yg(d)])

    order = fl["order"]
    units = [(half, o, d) for half in (1, 0) for d in range(4) for o in order]
    lag = fl["lag"]
    done = [0]
    def advance(k):
        while done[0] < min(k, len(units)):
            if fl["xy"]: xysend(*units[done[0]])
            done[0] += 1
    def relays(d):
        @pl.when(t == 0)
        def _():
            landed(1, 1, d)
            relay(d, 1, 1, 2)
        @pl.when(t == 1)
        def _():
            for o in (2, 3):
                landed(2, o, d)
                relay(d, o, 2, 1)
    for n, u in enumerate(units):
        advance(n + 1 + lag)
        half, o, d = u
        if half == 0 and n % 4 == 0 and fl["relay"]:
            relays(d)
        if o > 0:
            zsend(half, o, d)
        elif half == 1:
            if fl["xy"]: arrived(g.at[1, b, eight(d)], rxy.at[0, 1, yg(d)])
            if fl["relay"]:
                @pl.when(t == 0)
                def _():
                    relay(d, 0, 1, 2)

    if fl['relay']:
        @pl.when(t == 0)
        def _():
            for o in (2, 3):
                for d in range(4):
                    landed(1, o, d)

        @pl.when(t == 1)
        def _():
            for o in (0, 1):
                for d in range(4):
                    landed(2, o, d)
            for o in (2, 3, 1):
                for d in range(4):
                    landed(1, o, d)
    else:
        for o in (2,3,1):
            for d in range(4):
                landed(1, o, d)
    for d in range(4):
        if fl["xy"]: arrived(g.at[0, b, eight(d)], rxy.at[0, 0, yg(d)])
    for o in (2, 3, 1):
        for d in range(4):
            landed(0, o, d)
    for o in range(4):
        for half in range(2):
            if fl["xy"]: arrived(s.at[0, 0, pl.ds(0, 31)], sx.at[o, half])
            if o > 0:
                arrived(s.at[0, 0], sz.at[o, half])
    if fl['relay']:
        @pl.when(t == 0)
        def _():
            for o in (0, 1):
                arrived(s.at[0, 0], sr.at[o])
        @pl.when(t == 1)
        def _():
            for o in (2, 3):
                arrived(s.at[0, 0], sr.at[o])
    cp = pltpu.make_async_copy(g, out, fin)
    cp.start()
    cp.wait()


def comm(v):
    bf = jnp.bfloat16
    D = pltpu.SemaphoreType.DMA
    return pl.pallas_call(
        functools.partial(comm_kernel, dict(FL)),
        out_shape=jax.ShapeDtypeStruct((3, 4, 32, 2, 2, 8, 128), bf),
        in_specs=[pl.BlockSpec(memory_space=pl.ANY)],
        out_specs=pl.BlockSpec(memory_space=pl.ANY),
        scratch_shapes=[
            pltpu.VMEM((3, 2, 32, 2, 2, 8, 128), bf),
            pltpu.VMEM((3, 4, 32, 2, 2, 8, 128), bf),
            D((4, 2, 4)), D((3, 4, 4)), D((4, 2)), D((4, 2)), D((4,)), D,
        ],
        compiler_params=pltpu.CompilerParams(collective_id=0, has_side_effects=True),
    )(v)


HALF = 128


def tapers(length):
    steps = jnp.arange(length, dtype=jnp.float32)
    taper_early = jnp.sin(jnp.pi * (steps + 0.5) / (2.0 * length))
    taper_late = jnp.sin(jnp.pi * (steps + 0.5 + length) / (2.0 * length))
    return (taper_early, taper_late)


def weighted(block, taper):
    return (block.astype(jnp.float32) * taper).astype(jnp.bfloat16)


def local(voltages):
    g = comm(voltages.reshape(2, 2, 128, 8, 256))
    t = lax.axis_index("tm")
    x = g.transpose(0, 5, 3, 2, 1, 4, 6).reshape(3, 8, 2, 256, 128)
    early, late = tapers(HALF)
    zero = jnp.zeros((), jnp.bfloat16)
    tail = jnp.where(t == 1, weighted(x[2], early), zero)
    l0, l1, e0 = weighted(x[0], late), weighted(x[1], late), weighted(x[0], early)
    def win(lo, ea):
        a = jnp.concatenate([lo[:, 0], lo[:, 1], ea[:, 0], ea[:, 1]], -1)
        m = jnp.concatenate([lo[:, 1], -lo[:, 0], ea[:, 1], -ea[:, 0]], -1)
        re = jnp.einsum("cpk,cqk->cpq", a, a, preferred_element_type=jnp.float32)
        im = jnp.einsum("cpk,cqk->cpq", m, a, preferred_element_type=jnp.float32)
        return jnp.stack([re, im], 0) * (1.0 / HALF)
    return jnp.stack([win(l0, tail), win(l1, e0)], 2).astype(jnp.bfloat16)


def solution(mesh):
    return jax.shard_map(
        local,
        mesh=mesh,
        in_specs=(P(None, ("chan", "bl"), None, "tm"),),
        out_specs=P(None, ("chan", "bl"), "tm", None, None),
        check_vma=False,
    )
```

```python
import functools

import jax
import jax.numpy as jnp
import numpy as np
from jax import lax
from jax.sharding import PartitionSpec as P
from jax.experimental import pallas as pl
from jax.experimental.pallas import tpu as pltpu
MESH = pl.DeviceIdType.MESH
FL = dict(relay=True, order=(3, 1, 2, 0), lag=4, xy=True, odd=(0,2), first=((2, 1), (3, 1), (1, 1), (2, 3), (3, 3), (1, 3), (2, 2), (3, 2), (1, 2)), ds=(0,1,2,3), up=6, at=8, last=(1,3,2,0))

def comm_kernel(fl, v, pm, out, s, g, s1, ys, rxy, rz, sx, sz, sr, rf, sf, sg, fin):
    t, c, b = lax.axis_index("tm"), lax.axis_index("chan"), lax.axis_index("bl")
    y, l = lax.div(c, 8), lax.rem(c, 8)

    def piece(cc, bb, half):
        return v.at[:, :, cc, bb, :, pl.ds(half * 128, 128)]

    def spot(o, half, cc):
        return g.at[half, b, cc] if o == 0 else s.at[o - 1, half, cc]

    sem = pltpu.get_barrier_semaphore()
    def greet(**k):
        pl.semaphore_signal(sem, inc=1, device_id=k, device_id_type=MESH)
    for o in (2, 1, 3):
        greet(bl=lax.rem(b + o, 4))
    greet(tm=1 - t)
    far = jnp.where(t == 0, 1, -1)
    greet(tm=1 - t, bl=lax.rem(b - 2 * far + 8, 4))
    greet(tm=1 - t, bl=lax.rem(b - far + 8, 4))
    def greet_xy(i, _):
        greet(chan=lax.rem(c + i, 32))
        return 0
    lax.fori_loop(1, 32, greet_xy, 0)
    for half in (1, 0):
        for o in (2, 3, 1, 0):
            pltpu.make_async_copy(piece(c, lax.rem(b + o, 4), half), spot(o, half, c), rxy.at[o, half, y]).start()
    pl.semaphore_wait(sem, 37)
    if not fl["xy"]:
        for half in (1, 0):
            for o in range(4):
                pltpu.make_async_copy(piece(c, lax.rem(b + o, 4), half), spot(o, half, c), rxy.at[o, half, y]).wait()

    def xysend(half, o, d):
        def send(j, _):
            cc = lax.rem(y + d, 4) * 8 + lax.rem(l + j, 8)
            pltpu.make_async_remote_copy(
                src_ref=piece(cc, lax.rem(b + o, 4), half), dst_ref=spot(o, half, c),
                send_sem=sx.at[o, half], recv_sem=rxy.at[o, half, y],
                device_id={"chan": cc}, device_id_type=MESH).start()
            return 0
        lax.fori_loop(1 if d == 0 else 0, 8, send, 0)

    def rows(ref):
        return ref
    def arrived(ref, sm):
        pltpu.make_async_copy(ref, ref, sm).wait()

    def yg(d):
        return lax.rem(y + 4 - d, 4)
    def eight(d):
        return pl.ds(pl.multiple_of(yg(d) * 8, 8), 8)

    def via_odd(o, d):
        return o == 3 or (o == 2 and d in fl["odd"])

    def zsend(half, o, d):
        part = s.at[o - 1, half, eight(d)]
        if fl["xy"]: arrived(part, rxy.at[o, half, yg(d)])
        if half == 1 and via_odd(o, d) and fl["relay"]:
            to_t = jnp.int32(1)
            h = jnp.where(t == 0, 2, 1)
        else:
            to_t, h = t, half
        pltpu.make_async_remote_copy(
            src_ref=part, dst_ref=g.at[h, b, eight(d)],
            send_sem=sz.at[o, half], recv_sem=rz.at[h, o, yg(d)],
            device_id={"bl": lax.rem(b + o, 4), "tm": to_t}, device_id_type=MESH).start()

    def relay(d, o, h_from, h_to):
        src = lax.rem(b + 4 - o, 4)
        pltpu.make_async_remote_copy(
            src_ref=g.at[h_from, src, eight(d)], dst_ref=g.at[h_to, src, eight(d)],
            send_sem=sr.at[o, d], recv_sem=rz.at[h_to, o, yg(d)],
            device_id={"tm": 1 - t}, device_id_type=MESH).start()

    def landed(h, o, d):
        arrived(g.at[h, lax.rem(b + 4 - o, 4), eight(d)], rz.at[h, o, yg(d)])

    first = fl["first"]
    def far_send(o, d):
        row = pl.multiple_of(lax.rem(y + d, 4) * 8, 8)
        pltpu.make_async_remote_copy(
            src_ref=v.at[:, :, pl.ds(row, 8), lax.rem(b + o, 4), :, pl.ds(0, 128)],
            dst_ref=s1.at[first.index((o, d))],
            send_sem=sf.at[first.index((o, d))], recv_sem=rf.at[first.index((o, d))],
            device_id={"bl": lax.rem(b + o, 4)}, device_id_type=MESH).start()
    def far_pass(o, d):
        k = first.index((o, d))
        arrived(s1.at[k], rf.at[k])
        def send(j, _):
            lane = lax.rem(l + j, 8)
            pltpu.make_async_remote_copy(
                src_ref=s1.at[k, :, :, lane], dst_ref=g.at[0, lax.rem(b + 4 - o, 4), c],
                send_sem=sg.at[k], recv_sem=rz.at[0, o, y],
                device_id={"chan": lax.rem(y + d, 4) * 8 + lane}, device_id_type=MESH).start()
            return 0
        lax.fori_loop(0, 8, send, 0)
    up = fl["up"]
    for u in first[:up]:
        far_send(*u)
    order = fl["order"]
    units = [(half, o, d) for half in (1, 0) for d in fl["ds"] for o in order if half == 1 or (o, d) not in first]
    lag = fl["lag"]
    done = [0]
    def advance(k):
        while done[0] < min(k, len(units)):
            if fl["xy"]: xysend(*units[done[0]])
            done[0] += 1
    def relays(d):
        @pl.when(t == 0)
        def _():
            for o in (1, 2):
                if not via_odd(o, d):
                    landed(1, o, d)
                    relay(d, o, 1, 2)
        @pl.when(t == 1)
        def _():
            for o in (2, 3):
                if via_odd(o, d):
                    landed(2, o, d)
                    relay(d, o, 2, 1)
    for n, u in enumerate(units):
        advance(n + 1 + lag)
        if n == fl["at"]:
            for k in first[up:]:
                far_send(*k)
        half, o, d = u
        if half == 0 and units[n - 1][2] != d or n == 16 and fl["relay"]:
            if n == 16:
                for k in first:
                    far_pass(*k)
            relays(d)
        if o > 0:
            zsend(half, o, d)
        elif half == 1:
            if fl["xy"]: arrived(g.at[1, b, eight(d)], rxy.at[0, 1, yg(d)])
            if fl["relay"]:
                @pl.when(t == 0)
                def _():
                    relay(d, 0, 1, 2)

    def written(h, d):
        at = (h, slice(None), slice(None), pl.ds(pl.multiple_of(yg(d) * 64, 64), 64))
        return pltpu.make_async_copy(ys.at[at], out.at[at], fin.at[h, d])

    def settle(h, d):
        for k in range(2):
            for p in range(2):
                x = g[h, :, pl.ds(yg(d) * 8 + 4 * k, 4), p].reshape(256, 128)
                r = jnp.dot(pm[...], x, preferred_element_type=jnp.float32)
                r = r.astype(jnp.bfloat16).reshape(8, 32, 128)
                ys[h, :, p, pl.ds(pl.multiple_of(yg(d) * 64 + 32 * k, 32), 32), :] = r
        written(h, d).start()

    for d in range(4):
        @pl.when(t == 0)
        def _():
            for o in (2, 3):
                if via_odd(o, d):
                    landed(1, o, d)

        @pl.when(t == 1)
        def _():
            for o in (0, 1, 2):
                if not via_odd(o, d):
                    landed(2, o, d)
            settle(2, d)
            for o in (2, 3, 1):
                landed(1, o, d)
        settle(1, d)
    for d in fl["last"]:
        arrived(g.at[0, b, eight(d)], rxy.at[0, 0, yg(d)])
        for o in (2, 3, 1):
            landed(0, o, d)
        settle(0, d)
    for o in range(4):
        for half in range(2):
            gone = [d for (oo, d) in first if oo == o] if half == 0 else []
            if fl["xy"]: arrived(s.at[0, 0, pl.ds(0, 31 - 8 * len(gone))], sx.at[o, half])
            if o > 0:
                arrived(s.at[0, 0, pl.ds(0, 32 - 8 * len(gone))], sz.at[o, half])
    if fl['relay']:
        for o in range(4):
            for d in range(4):
                @pl.when(t == (1 if via_odd(o, d) else 0))
                def _():
                    arrived(s.at[0, 0, pl.ds(0, 8)], sr.at[o, d])
    for k in range(len(first)):
        arrived(s1.at[k], sf.at[k])
        arrived(s1.at[k], sg.at[k])
    for d in range(4):
        written(1, d).wait()
        written(0, d).wait()

        @pl.when(t == 1)
        def _():
            written(2, d).wait()


def comm(v, pm):
    bf = jnp.bfloat16
    D = pltpu.SemaphoreType.DMA
    return pl.pallas_call(
        functools.partial(comm_kernel, dict(FL)),
        out_shape=jax.ShapeDtypeStruct((3, 8, 2, 256, 128), bf),
        in_specs=[pl.BlockSpec(memory_space=pl.ANY), pl.BlockSpec(memory_space=pltpu.VMEM)],
        out_specs=pl.BlockSpec(memory_space=pl.ANY),
        scratch_shapes=[
            pltpu.VMEM((3, 2, 32, 2, 2, 8, 128), bf),
            pltpu.VMEM((3, 4, 32, 2, 2, 8, 128), bf),
            pltpu.VMEM((max(1, len(FL["first"])), 2, 2, 8, 8, 128), bf),
            pltpu.VMEM((3, 8, 2, 256, 128), bf),
            D((4, 2, 4)), D((3, 4, 4)), D((4, 2)), D((4, 2)), D((4, 4)), D((12,)), D((12,)), D((12,)), D((3, 4)),
        ],
        compiler_params=pltpu.CompilerParams(collective_id=0, has_side_effects=True),
        name="gather",
    )(v.reshape(2, 2, 32, 4, 8, 256), pm)


def corr_kernel(tap, y_ref, o_ref):
    early, late = tap[0:1, :], tap[1:2, :]
    t = lax.axis_index("tm")
    f32, bf = jnp.float32, jnp.bfloat16

    def load(h, p):
        return y_ref[h, 0, p].astype(f32)

    def window(w, lo, ea):
        al, bl_, ae, be = lo[0], lo[1], ea[0], ea[1]
        rhs = jnp.concatenate([al, bl_, ae, be], 1)
        lhs = jnp.concatenate([bl_, -al, be, -ae], 1)
        for i, m in enumerate((rhs, lhs)):
            r = lax.dot_general(m, rhs, (((1,), (1,)), ((), ())), preferred_element_type=f32)
            o_ref[i, 0, w] = (r * (1.0 / 128)).astype(bf)

    a = [load(0, p) for p in (0, 1)]
    tail = [(load(2, p) * early) for p in (0, 1)]
    tail = [jnp.where(t == 1, x, 0.0).astype(bf) for x in tail]
    window(0, [(x * late).astype(bf) for x in a], tail)
    bb = [load(1, p) for p in (0, 1)]
    window(1, [(x * late).astype(bf) for x in bb], [(x * early).astype(bf) for x in a])


def corr(tap, y):
    return pl.pallas_call(
        corr_kernel,
        grid=(8,),
        out_shape=jax.ShapeDtypeStruct((2, 8, 2, 256, 256), jnp.bfloat16),
        in_specs=[
            pl.BlockSpec((2, 128), lambda i: (0, 0)),
            pl.BlockSpec((3, 1, 2, 256, 128), lambda i: (0, i, 0, 0, 0)),
        ],
        out_specs=pl.BlockSpec((2, 1, 2, 256, 256), lambda i: (0, i, 0, 0, 0)),
        compiler_params=pltpu.CompilerParams(dimension_semantics=("arbitrary",)),
        name="corr",
    )(tap, y)


def tapers():
    steps = np.arange(128, dtype=np.float64)
    return np.stack([np.sin(np.pi * (steps + 0.5) / 256), np.sin(np.pi * (steps + 128.5) / 256)]).astype(np.float32)


def perm():
    m = np.zeros((256, 256), np.float32)
    for b in range(4):
        for c in range(4):
            for s in range(2):
                for h in range(8):
                    m[h * 32 + c * 8 + b * 2 + s, ((b * 4 + c) * 2 + s) * 8 + h] = 1
    return m


def local(voltages):
    y = comm(voltages.reshape(2, 2, 128, 8, 256), perm().astype(jnp.bfloat16))
    return corr(tapers(), y)


def solution(mesh):
    return jax.shard_map(
        local,
        mesh=mesh,
        in_specs=(P(None, ("chan", "bl"), None, "tm"),),
        out_specs=P(None, ("chan", "bl"), "tm", None, None),
        check_vma=False,
    )
```

```python
import functools

import jax
import jax.numpy as jnp
import numpy as np
from jax import lax
from jax.sharding import PartitionSpec as P
from jax.experimental import pallas as pl
from jax.experimental.pallas import tpu as pltpu
MESH = pl.DeviceIdType.MESH
FL = dict(relay=True, order=(3, 1, 2, 0), lag=4, xy=True, odd=(0,2), first=((2, 1), (3, 1), (1, 1), (2, 3), (3, 3), (1, 3), (2, 2), (3, 2), (1, 2)), ds=(0,1,2,3), up=6, at=8, last=(1,3,2,0))

def comm_kernel(fl, v, pm, ys, s, g, s1, rxy, rz, sx, sz, sr, rf, sf, sg):
    t, c, b = lax.axis_index("tm"), lax.axis_index("chan"), lax.axis_index("bl")
    y, l = lax.div(c, 8), lax.rem(c, 8)

    def piece(cc, bb, half):
        return v.at[:, :, cc, bb, :, pl.ds(half * 128, 128)]

    def spot(o, half, cc):
        return g.at[half, b, cc] if o == 0 else s.at[o - 1, half, cc]

    sem = pltpu.get_barrier_semaphore()
    def greet(**k):
        pl.semaphore_signal(sem, inc=1, device_id=k, device_id_type=MESH)
    for o in (2, 1, 3):
        greet(bl=lax.rem(b + o, 4))
    greet(tm=1 - t)
    far = jnp.where(t == 0, 1, -1)
    greet(tm=1 - t, bl=lax.rem(b - 2 * far + 8, 4))
    greet(tm=1 - t, bl=lax.rem(b - far + 8, 4))
    def greet_xy(i, _):
        greet(chan=lax.rem(c + i, 32))
        return 0
    lax.fori_loop(1, 32, greet_xy, 0)
    for half in (1, 0):
        for o in (2, 3, 1, 0):
            pltpu.make_async_copy(piece(c, lax.rem(b + o, 4), half), spot(o, half, c), rxy.at[o, half, y]).start()
    pl.semaphore_wait(sem, 37)
    if not fl["xy"]:
        for half in (1, 0):
            for o in range(4):
                pltpu.make_async_copy(piece(c, lax.rem(b + o, 4), half), spot(o, half, c), rxy.at[o, half, y]).wait()

    def xysend(half, o, d):
        def send(j, _):
            cc = lax.rem(y + d, 4) * 8 + lax.rem(l + j, 8)
            pltpu.make_async_remote_copy(
                src_ref=piece(cc, lax.rem(b + o, 4), half), dst_ref=spot(o, half, c),
                send_sem=sx.at[o, half], recv_sem=rxy.at[o, half, y],
                device_id={"chan": cc}, device_id_type=MESH).start()
            return 0
        lax.fori_loop(1 if d == 0 else 0, 8, send, 0)

    def rows(ref):
        return ref
    def arrived(ref, sm):
        pltpu.make_async_copy(ref, ref, sm).wait()

    def yg(d):
        return lax.rem(y + 4 - d, 4)
    def eight(d):
        return pl.ds(pl.multiple_of(yg(d) * 8, 8), 8)

    def via_odd(o, d):
        return o == 3 or (o == 2 and d in fl["odd"])

    def zsend(half, o, d):
        part = s.at[o - 1, half, eight(d)]
        if fl["xy"]: arrived(part, rxy.at[o, half, yg(d)])
        if half == 1 and via_odd(o, d) and fl["relay"]:
            to_t = jnp.int32(1)
            h = jnp.where(t == 0, 2, 1)
        else:
            to_t, h = t, half
        pltpu.make_async_remote_copy(
            src_ref=part, dst_ref=g.at[h, b, eight(d)],
            send_sem=sz.at[o, half], recv_sem=rz.at[h, o, yg(d)],
            device_id={"bl": lax.rem(b + o, 4), "tm": to_t}, device_id_type=MESH).start()

    def relay(d, o, h_from, h_to):
        src = lax.rem(b + 4 - o, 4)
        pltpu.make_async_remote_copy(
            src_ref=g.at[h_from, src, eight(d)], dst_ref=g.at[h_to, src, eight(d)],
            send_sem=sr.at[o, d], recv_sem=rz.at[h_to, o, yg(d)],
            device_id={"tm": 1 - t}, device_id_type=MESH).start()

    def landed(h, o, d):
        arrived(g.at[h, lax.rem(b + 4 - o, 4), eight(d)], rz.at[h, o, yg(d)])

    first = fl["first"]
    def far_send(o, d):
        row = pl.multiple_of(lax.rem(y + d, 4) * 8, 8)
        pltpu.make_async_remote_copy(
            src_ref=v.at[:, :, pl.ds(row, 8), lax.rem(b + o, 4), :, pl.ds(0, 128)],
            dst_ref=s1.at[first.index((o, d))],
            send_sem=sf.at[first.index((o, d))], recv_sem=rf.at[first.index((o, d))],
            device_id={"bl": lax.rem(b + o, 4)}, device_id_type=MESH).start()
    def far_pass(o, d):
        k = first.index((o, d))
        arrived(s1.at[k], rf.at[k])
        def send(j, _):
            lane = lax.rem(l + j, 8)
            pltpu.make_async_remote_copy(
                src_ref=s1.at[k, :, :, lane], dst_ref=g.at[0, lax.rem(b + 4 - o, 4), c],
                send_sem=sg.at[k], recv_sem=rz.at[0, o, y],
                device_id={"chan": lax.rem(y + d, 4) * 8 + lane}, device_id_type=MESH).start()
            return 0
        lax.fori_loop(0, 8, send, 0)
    up = fl["up"]
    for u in first[:up]:
        far_send(*u)
    order = fl["order"]
    units = [(half, o, d) for half in (1, 0) for d in fl["ds"] for o in order if half == 1 or (o, d) not in first]
    lag = fl["lag"]
    done = [0]
    def advance(k):
        while done[0] < min(k, len(units)):
            if fl["xy"]: xysend(*units[done[0]])
            done[0] += 1
    def relays(d):
        @pl.when(t == 0)
        def _():
            for o in (1, 2):
                if not via_odd(o, d):
                    landed(1, o, d)
                    relay(d, o, 1, 2)
        @pl.when(t == 1)
        def _():
            for o in (2, 3):
                if via_odd(o, d):
                    landed(2, o, d)
                    relay(d, o, 2, 1)
    for n, u in enumerate(units):
        advance(n + 1 + lag)
        if n == fl["at"]:
            for k in first[up:]:
                far_send(*k)
        half, o, d = u
        if half == 0 and units[n - 1][2] != d or n == 16 and fl["relay"]:
            if n == 16:
                for k in first:
                    far_pass(*k)
            relays(d)
        if o > 0:
            zsend(half, o, d)
        elif half == 1:
            if fl["xy"]: arrived(g.at[1, b, eight(d)], rxy.at[0, 1, yg(d)])
            if fl["relay"]:
                @pl.when(t == 0)
                def _():
                    relay(d, 0, 1, 2)

    def settle(h, d):
        for k in range(2):
            for p in range(2):
                x = g[h, :, pl.ds(yg(d) * 8 + 4 * k, 4), p].reshape(256, 128)
                r = jnp.dot(pm[...], x, preferred_element_type=jnp.float32)
                r = r.astype(jnp.bfloat16).reshape(8, 32, 128)
                ys[h, :, p, pl.ds(pl.multiple_of(yg(d) * 64 + 32 * k, 32), 32), :] = r

    for d in range(4):
        @pl.when(t == 0)
        def _():
            for o in (2, 3):
                if via_odd(o, d):
                    landed(1, o, d)

        @pl.when(t == 1)
        def _():
            for o in (0, 1, 2):
                if not via_odd(o, d):
                    landed(2, o, d)
            settle(2, d)
            for o in (2, 3, 1):
                landed(1, o, d)
        settle(1, d)
    for d in fl["last"]:
        arrived(g.at[0, b, eight(d)], rxy.at[0, 0, yg(d)])
        for o in (2, 3, 1):
            landed(0, o, d)
        settle(0, d)
    for o in range(4):
        for half in range(2):
            gone = [d for (oo, d) in first if oo == o] if half == 0 else []
            if fl["xy"]: arrived(s.at[0, 0, pl.ds(0, 31 - 8 * len(gone))], sx.at[o, half])
            if o > 0:
                arrived(s.at[0, 0, pl.ds(0, 32 - 8 * len(gone))], sz.at[o, half])
    if fl['relay']:
        for o in range(4):
            for d in range(4):
                @pl.when(t == (1 if via_odd(o, d) else 0))
                def _():
                    arrived(s.at[0, 0, pl.ds(0, 8)], sr.at[o, d])
    for k in range(len(first)):
        arrived(s1.at[k], sf.at[k])
        arrived(s1.at[k], sg.at[k])


def comm(v, pm):
    bf = jnp.bfloat16
    D = pltpu.SemaphoreType.DMA
    return pl.pallas_call(
        functools.partial(comm_kernel, dict(FL)),
        out_shape=pltpu.VMEM((3, 8, 2, 256, 128), bf),
        in_specs=[pl.BlockSpec(memory_space=pl.ANY), pl.BlockSpec(memory_space=pltpu.VMEM)],
        out_specs=pl.BlockSpec(memory_space=pltpu.VMEM),
        scratch_shapes=[
            pltpu.VMEM((3, 2, 32, 2, 2, 8, 128), bf),
            pltpu.VMEM((3, 4, 32, 2, 2, 8, 128), bf),
            pltpu.VMEM((max(1, len(FL["first"])), 2, 2, 8, 8, 128), bf),
            D((4, 2, 4)), D((3, 4, 4)), D((4, 2)), D((4, 2)), D((4, 4)), D((12,)), D((12,)), D((12,)),
        ],
        compiler_params=pltpu.CompilerParams(collective_id=0, has_side_effects=True),
        name="gather",
    )(v.reshape(2, 2, 32, 4, 8, 256), pm)


N = 4


def corr_kernel(tap, y_ref, o_ref):
    for n in range(N):
        one(tap, y_ref, o_ref, n)


def one(tap, y_ref, o_ref, n):
    ch = pl.program_id(0) * N + n
    early, late = tap[0:1, :], tap[1:2, :]
    t = lax.axis_index("tm")
    f32, bf = jnp.float32, jnp.bfloat16

    def load(h, p):
        return y_ref[h, ch, p].astype(f32)

    def window(w, lo, ea):
        al, bl_, ae, be = lo[0], lo[1], ea[0], ea[1]
        rhs = jnp.concatenate([al, bl_, ae, be], 1)
        lhs = jnp.concatenate([bl_, -al, be, -ae], 1)
        for i, m in enumerate((rhs, lhs)):
            r = lax.dot_general(m, rhs, (((1,), (1,)), ((), ())), preferred_element_type=f32)
            o_ref[i, n, w] = (r * (1.0 / 128)).astype(bf)

    a = [load(0, p) for p in (0, 1)]
    tail = [(load(2, p) * early) for p in (0, 1)]
    tail = [jnp.where(t == 1, x, 0.0).astype(bf) for x in tail]
    window(0, [(x * late).astype(bf) for x in a], tail)
    bb = [load(1, p) for p in (0, 1)]
    window(1, [(x * late).astype(bf) for x in bb], [(x * early).astype(bf) for x in a])


def corr(tap, y):
    return pl.pallas_call(
        corr_kernel,
        grid=(8 // N,),
        out_shape=jax.ShapeDtypeStruct((2, 8, 2, 256, 256), jnp.bfloat16),
        in_specs=[
            pl.BlockSpec((2, 128), lambda i: (0, 0)),
            pl.BlockSpec(memory_space=pltpu.VMEM),
        ],
        out_specs=pl.BlockSpec((2, N, 2, 256, 256), lambda i: (0, i, 0, 0, 0)),
        compiler_params=pltpu.CompilerParams(dimension_semantics=("arbitrary",), vmem_limit_bytes=24 * 2**20),
        name="corr",
    )(tap, y)


def tapers():
    steps = np.arange(128, dtype=np.float64)
    return np.stack([np.sin(np.pi * (steps + 0.5) / 256), np.sin(np.pi * (steps + 128.5) / 256)]).astype(np.float32)


def perm():
    m = np.zeros((256, 256), np.float32)
    for b in range(4):
        for c in range(4):
            for s in range(2):
                for h in range(8):
                    m[h * 32 + c * 8 + b * 2 + s, ((b * 4 + c) * 2 + s) * 8 + h] = 1
    return m


def local(voltages):
    y = comm(voltages.reshape(2, 2, 128, 8, 256), perm().astype(jnp.bfloat16))
    return corr(tapers(), y)


def solution(mesh):
    return jax.shard_map(
        local,
        mesh=mesh,
        in_specs=(P(None, ("chan", "bl"), None, "tm"),),
        out_specs=P(None, ("chan", "bl"), "tm", None, None),
        check_vma=False,
    )
```

```python
import functools

import jax
import jax.numpy as jnp
import numpy as np
from jax import lax
from jax.sharding import PartitionSpec as P
from jax.experimental import pallas as pl
from jax.experimental.pallas import tpu as pltpu
MESH = pl.DeviceIdType.MESH
FL = dict(relay=True, order=(3, 1, 2, 0), lag=4, xy=True, odd=(0,2), first=((2, 1), (3, 1), (1, 1), (2, 3), (3, 3), (1, 3), (2, 2), (3, 2), (1, 2)), ds=(0,1,2,3), up=6, at=8, last=(1,3,2,0))

def comm_kernel(fl, v, pm, ys, s, g, s1, rxy, rz, sx, sz, sr, rf, sf, sg):
    t, c, b = lax.axis_index("tm"), lax.axis_index("chan"), lax.axis_index("bl")
    y, l = lax.div(c, 8), lax.rem(c, 8)

    def piece(cc, bb, half):
        return v.at[:, :, cc, bb, :, pl.ds(half * 128, 128)]

    def spot(o, half, cc):
        return g.at[half, b, cc] if o == 0 else s.at[o - 1, half, cc]

    sem = pltpu.get_barrier_semaphore()
    def greet(**k):
        pl.semaphore_signal(sem, inc=1, device_id=k, device_id_type=MESH)
    for o in (2, 1, 3):
        greet(bl=lax.rem(b + o, 4))
    greet(tm=1 - t)
    far = jnp.where(t == 0, 1, -1)
    greet(tm=1 - t, bl=lax.rem(b - 2 * far + 8, 4))
    greet(tm=1 - t, bl=lax.rem(b - far + 8, 4))
    def greet_xy(i, _):
        greet(chan=lax.rem(c + i, 32))
        return 0
    lax.fori_loop(1, 32, greet_xy, 0)
    for half in (1, 0):
        for o in (2, 3, 1, 0):
            pltpu.make_async_copy(piece(c, lax.rem(b + o, 4), half), spot(o, half, c), rxy.at[o, half, y]).start()
    pl.semaphore_wait(sem, 37)
    if not fl["xy"]:
        for half in (1, 0):
            for o in range(4):
                pltpu.make_async_copy(piece(c, lax.rem(b + o, 4), half), spot(o, half, c), rxy.at[o, half, y]).wait()

    def xysend(half, o, d):
        def send(j, _):
            cc = lax.rem(y + d, 4) * 8 + lax.rem(l + j, 8)
            pltpu.make_async_remote_copy(
                src_ref=piece(cc, lax.rem(b + o, 4), half), dst_ref=spot(o, half, c),
                send_sem=sx.at[o, half], recv_sem=rxy.at[o, half, y],
                device_id={"chan": cc}, device_id_type=MESH).start()
            return 0
        lax.fori_loop(1 if d == 0 else 0, 8, send, 0)

    def rows(ref):
        return ref
    def arrived(ref, sm):
        pltpu.make_async_copy(ref, ref, sm).wait()

    def yg(d):
        return lax.rem(y + 4 - d, 4)
    def eight(d):
        return pl.ds(pl.multiple_of(yg(d) * 8, 8), 8)

    def via_odd(o, d):
        return o == 3 or (o == 2 and d in fl["odd"])

    def zsend(half, o, d):
        part = s.at[o - 1, half, eight(d)]
        if fl["xy"]: arrived(part, rxy.at[o, half, yg(d)])
        if half == 1 and via_odd(o, d) and fl["relay"]:
            to_t = jnp.int32(1)
            h = jnp.where(t == 0, 2, 1)
        else:
            to_t, h = t, half
        pltpu.make_async_remote_copy(
            src_ref=part, dst_ref=g.at[h, b, eight(d)],
            send_sem=sz.at[o, half], recv_sem=rz.at[h, o, yg(d)],
            device_id={"bl": lax.rem(b + o, 4), "tm": to_t}, device_id_type=MESH).start()

    def relay(d, o, h_from, h_to):
        src = lax.rem(b + 4 - o, 4)
        pltpu.make_async_remote_copy(
            src_ref=g.at[h_from, src, eight(d)], dst_ref=g.at[h_to, src, eight(d)],
            send_sem=sr.at[o, d], recv_sem=rz.at[h_to, o, yg(d)],
            device_id={"tm": 1 - t}, device_id_type=MESH).start()

    def landed(h, o, d):
        arrived(g.at[h, lax.rem(b + 4 - o, 4), eight(d)], rz.at[h, o, yg(d)])

    first = fl["first"]
    def far_send(o, d):
        row = pl.multiple_of(lax.rem(y + d, 4) * 8, 8)
        pltpu.make_async_remote_copy(
            src_ref=v.at[:, :, pl.ds(row, 8), lax.rem(b + o, 4), :, pl.ds(0, 128)],
            dst_ref=s1.at[first.index((o, d))],
            send_sem=sf.at[first.index((o, d))], recv_sem=rf.at[first.index((o, d))],
            device_id={"bl": lax.rem(b + o, 4)}, device_id_type=MESH).start()
    def far_pass(o, d):
        k = first.index((o, d))
        arrived(s1.at[k], rf.at[k])
        def send(j, _):
            lane = lax.rem(l + j, 8)
            pltpu.make_async_remote_copy(
                src_ref=s1.at[k, :, :, lane], dst_ref=g.at[0, lax.rem(b + 4 - o, 4), c],
                send_sem=sg.at[k], recv_sem=rz.at[0, o, y],
                device_id={"chan": lax.rem(y + d, 4) * 8 + lane}, device_id_type=MESH).start()
            return 0
        lax.fori_loop(0, 8, send, 0)
    up = fl["up"]
    for u in first[:up]:
        far_send(*u)
    order = fl["order"]
    units = [(half, o, d) for half in (1, 0) for d in fl["ds"] for o in order if half == 1 or (o, d) not in first]
    lag = fl["lag"]
    done = [0]
    def advance(k):
        while done[0] < min(k, len(units)):
            if fl["xy"]: xysend(*units[done[0]])
            done[0] += 1
    def relays(d):
        @pl.when(t == 0)
        def _():
            for o in (1, 2):
                if not via_odd(o, d):
                    landed(1, o, d)
                    relay(d, o, 1, 2)
        @pl.when(t == 1)
        def _():
            for o in (2, 3):
                if via_odd(o, d):
                    landed(2, o, d)
                    relay(d, o, 2, 1)
    for n, u in enumerate(units):
        advance(n + 1 + lag)
        if n == fl["at"]:
            for k in first[up:]:
                far_send(*k)
        half, o, d = u
        if half == 0 and units[n - 1][2] != d or n == 16 and fl["relay"]:
            if n == 16:
                for k in first:
                    far_pass(*k)
            relays(d)
        if o > 0:
            zsend(half, o, d)
        elif half == 1:
            if fl["xy"]: arrived(g.at[1, b, eight(d)], rxy.at[0, 1, yg(d)])
            if fl["relay"]:
                @pl.when(t == 0)
                def _():
                    relay(d, 0, 1, 2)

    def settle(h, d):
        for k in range(2):
            for p in range(2):
                x = g[h, :, pl.ds(yg(d) * 8 + 4 * k, 4), p].reshape(256, 128)
                r = jnp.dot(pm[...], x, preferred_element_type=jnp.float32)
                r = r.astype(jnp.bfloat16).reshape(8, 32, 128)
                ys[h, :, p, pl.ds(pl.multiple_of(yg(d) * 64 + 32 * k, 32), 32), :] = r

    for d in range(4):
        @pl.when(t == 0)
        def _():
            for o in (2, 3):
                if via_odd(o, d):
                    landed(1, o, d)

        @pl.when(t == 1)
        def _():
            for o in (0, 1, 2):
                if not via_odd(o, d):
                    landed(2, o, d)
            settle(2, d)
            for o in (2, 3, 1):
                landed(1, o, d)
        settle(1, d)
    for d in fl["last"]:
        arrived(g.at[0, b, eight(d)], rxy.at[0, 0, yg(d)])
        for o in (2, 3, 1):
            landed(0, o, d)
        settle(0, d)
    for o in range(4):
        for half in range(2):
            gone = [d for (oo, d) in first if oo == o] if half == 0 else []
            if fl["xy"]: arrived(s.at[0, 0, pl.ds(0, 31 - 8 * len(gone))], sx.at[o, half])
            if o > 0:
                arrived(s.at[0, 0, pl.ds(0, 32 - 8 * len(gone))], sz.at[o, half])
    if fl['relay']:
        for o in range(4):
            for d in range(4):
                @pl.when(t == (1 if via_odd(o, d) else 0))
                def _():
                    arrived(s.at[0, 0, pl.ds(0, 8)], sr.at[o, d])
    for k in range(len(first)):
        arrived(s1.at[k], sf.at[k])
        arrived(s1.at[k], sg.at[k])


def comm(v, pm):
    bf = jnp.bfloat16
    D = pltpu.SemaphoreType.DMA
    return pl.pallas_call(
        functools.partial(comm_kernel, dict(FL)),
        out_shape=pltpu.VMEM((3, 8, 2, 256, 128), bf),
        in_specs=[pl.BlockSpec(memory_space=pl.ANY), pl.BlockSpec(memory_space=pltpu.VMEM)],
        out_specs=pl.BlockSpec(memory_space=pltpu.VMEM),
        scratch_shapes=[
            pltpu.VMEM((3, 2, 32, 2, 2, 8, 128), bf),
            pltpu.VMEM((3, 4, 32, 2, 2, 8, 128), bf),
            pltpu.VMEM((max(1, len(FL["first"])), 2, 2, 8, 8, 128), bf),
            D((4, 2, 4)), D((3, 4, 4)), D((4, 2)), D((4, 2)), D((4, 4)), D((12,)), D((12,)), D((12,)),
        ],
        compiler_params=pltpu.CompilerParams(collective_id=0, has_side_effects=True),
        name="gather",
    )(v.reshape(2, 2, 32, 4, 8, 256), pm)


def corr_kernel(tap, y_ref, out, o_ref, sem):
    def leave(n):
        return pltpu.make_async_copy(o_ref.at[:, n], out.at[:, n], sem.at[n])

    for n in range(8):
        one(tap, y_ref, o_ref, n)
        leave(n).start()
    for n in range(8):
        leave(n).wait()


def one(tap, y_ref, o_ref, n):
    ch = n
    early, late = tap[0:1, :], tap[1:2, :]
    t = lax.axis_index("tm")
    f32, bf = jnp.float32, jnp.bfloat16

    def load(h, p):
        return y_ref[h, ch, p].astype(f32)

    def window(w, lo, ea):
        al, bl_, ae, be = lo[0], lo[1], ea[0], ea[1]
        rhs = jnp.concatenate([al, bl_, ae, be], 1)
        lhs = jnp.concatenate([bl_, -al, be, -ae], 1)
        for i, m in enumerate((rhs, lhs)):
            r = lax.dot_general(m, rhs, (((1,), (1,)), ((), ())), preferred_element_type=f32)
            o_ref[i, n, w] = (r * (1.0 / 128)).astype(bf)

    a = [load(0, p) for p in (0, 1)]
    tail = [(load(2, p) * early) for p in (0, 1)]
    tail = [jnp.where(t == 1, x, 0.0).astype(bf) for x in tail]
    window(0, [(x * late).astype(bf) for x in a], tail)
    bb = [load(1, p) for p in (0, 1)]
    window(1, [(x * late).astype(bf) for x in bb], [(x * early).astype(bf) for x in a])


def corr(tap, y):
    return pl.pallas_call(
        corr_kernel,
        out_shape=jax.ShapeDtypeStruct((2, 8, 2, 256, 256), jnp.bfloat16),
        in_specs=[pl.BlockSpec(memory_space=pltpu.VMEM)] * 2,
        out_specs=pl.BlockSpec(memory_space=pl.ANY),
        scratch_shapes=[
            pltpu.VMEM((2, 8, 2, 256, 256), jnp.bfloat16),
            pltpu.SemaphoreType.DMA((8,)),
        ],
        compiler_params=pltpu.CompilerParams(vmem_limit_bytes=24 * 2**20),
        name="corr",
    )(tap, y)


def tapers():
    steps = np.arange(128, dtype=np.float64)
    return np.stack([np.sin(np.pi * (steps + 0.5) / 256), np.sin(np.pi * (steps + 128.5) / 256)]).astype(np.float32)


def perm():
    m = np.zeros((256, 256), np.float32)
    for b in range(4):
        for c in range(4):
            for s in range(2):
                for h in range(8):
                    m[h * 32 + c * 8 + b * 2 + s, ((b * 4 + c) * 2 + s) * 8 + h] = 1
    return m


def local(voltages):
    y = comm(voltages.reshape(2, 2, 128, 8, 256), perm().astype(jnp.bfloat16))
    return corr(tapers(), y)


def solution(mesh):
    return jax.shard_map(
        local,
        mesh=mesh,
        in_specs=(P(None, ("chan", "bl"), None, "tm"),),
        out_specs=P(None, ("chan", "bl"), "tm", None, None),
        check_vma=False,
    )
```

```python
import functools

import jax
import jax.numpy as jnp
import numpy as np
from jax import lax
from jax.sharding import PartitionSpec as P
from jax.experimental import pallas as pl
from jax.experimental.pallas import tpu as pltpu
MESH = pl.DeviceIdType.MESH
FL = dict(relay=True, order=(3, 1, 2, 0), lag=4, xy=True, odd=(0,2), first=((2, 1), (3, 1), (1, 1), (2, 3), (3, 3), (1, 3), (2, 2), (3, 2), (1, 2)), ds=(0,1,2,3), up=6, at=8, last=(1,3,2,0))

def comm_kernel(fl, v, pm, ys, s, g, s1, rxy, rz, sx, sz, sr, rf, sf, sg):
    t, c, b = lax.axis_index("tm"), lax.axis_index("chan"), lax.axis_index("bl")
    y, l = lax.div(c, 8), lax.rem(c, 8)

    def piece(cc, bb, half):
        return v.at[:, :, cc, bb, :, pl.ds(half * 128, 128)]

    def spot(o, half, cc):
        return g.at[half, b, cc] if o == 0 else s.at[o - 1, half, cc]

    sem = pltpu.get_barrier_semaphore()
    def greet(**k):
        pl.semaphore_signal(sem, inc=1, device_id=k, device_id_type=MESH)
    for o in (2, 1, 3):
        greet(bl=lax.rem(b + o, 4))
    greet(tm=1 - t)
    far = jnp.where(t == 0, 1, -1)
    greet(tm=1 - t, bl=lax.rem(b - 2 * far + 8, 4))
    greet(tm=1 - t, bl=lax.rem(b - far + 8, 4))
    def greet_xy(i, _):
        greet(chan=lax.rem(c + i, 32))
        return 0
    lax.fori_loop(1, 32, greet_xy, 0)
    for half in (1, 0):
        for o in (2, 3, 1, 0):
            pltpu.make_async_copy(piece(c, lax.rem(b + o, 4), half), spot(o, half, c), rxy.at[o, half, y]).start()
    pl.semaphore_wait(sem, 37)
    if not fl["xy"]:
        for half in (1, 0):
            for o in range(4):
                pltpu.make_async_copy(piece(c, lax.rem(b + o, 4), half), spot(o, half, c), rxy.at[o, half, y]).wait()

    def xysend(half, o, d):
        def send(j, _):
            cc = lax.rem(y + d, 4) * 8 + lax.rem(l + j, 8)
            pltpu.make_async_remote_copy(
                src_ref=piece(cc, lax.rem(b + o, 4), half), dst_ref=spot(o, half, c),
                send_sem=sx.at[o, half], recv_sem=rxy.at[o, half, y],
                device_id={"chan": cc}, device_id_type=MESH).start()
            return 0
        lax.fori_loop(1 if d == 0 else 0, 8, send, 0)

    def rows(ref):
        return ref
    def arrived(ref, sm):
        pltpu.make_async_copy(ref, ref, sm).wait()

    def yg(d):
        return lax.rem(y + 4 - d, 4)
    def eight(d):
        return pl.ds(pl.multiple_of(yg(d) * 8, 8), 8)

    def via_odd(o, d):
        return o == 3 or (o == 2 and d in fl["odd"])

    def zsend(half, o, d):
        part = s.at[o - 1, half, eight(d)]
        if fl["xy"]: arrived(part, rxy.at[o, half, yg(d)])
        if half == 1 and via_odd(o, d) and fl["relay"]:
            to_t = jnp.int32(1)
            h = jnp.where(t == 0, 2, 1)
        else:
            to_t, h = t, half
        pltpu.make_async_remote_copy(
            src_ref=part, dst_ref=g.at[h, b, eight(d)],
            send_sem=sz.at[o, half], recv_sem=rz.at[h, o, yg(d)],
            device_id={"bl": lax.rem(b + o, 4), "tm": to_t}, device_id_type=MESH).start()

    def relay(d, o, h_from, h_to):
        src = lax.rem(b + 4 - o, 4)
        pltpu.make_async_remote_copy(
            src_ref=g.at[h_from, src, eight(d)], dst_ref=g.at[h_to, src, eight(d)],
            send_sem=sr.at[o, d], recv_sem=rz.at[h_to, o, yg(d)],
            device_id={"tm": 1 - t}, device_id_type=MESH).start()

    def landed(h, o, d):
        arrived(g.at[h, lax.rem(b + 4 - o, 4), eight(d)], rz.at[h, o, yg(d)])

    first = fl["first"]
    def far_send(o, d):
        row = pl.multiple_of(lax.rem(y + d, 4) * 8, 8)
        pltpu.make_async_remote_copy(
            src_ref=v.at[:, :, pl.ds(row, 8), lax.rem(b + o, 4), :, pl.ds(0, 128)],
            dst_ref=s1.at[first.index((o, d))],
            send_sem=sf.at[first.index((o, d))], recv_sem=rf.at[first.index((o, d))],
            device_id={"bl": lax.rem(b + o, 4)}, device_id_type=MESH).start()
    def far_pass(o, d):
        k = first.index((o, d))
        arrived(s1.at[k], rf.at[k])
        def send(j, _):
            lane = lax.rem(l + j, 8)
            pltpu.make_async_remote_copy(
                src_ref=s1.at[k, :, :, lane], dst_ref=g.at[0, lax.rem(b + 4 - o, 4), c],
                send_sem=sg.at[k], recv_sem=rz.at[0, o, y],
                device_id={"chan": lax.rem(y + d, 4) * 8 + lane}, device_id_type=MESH).start()
            return 0
        lax.fori_loop(0, 8, send, 0)
    up = fl["up"]
    for u in first[:up]:
        far_send(*u)
    order = fl["order"]
    units = [(half, o, d) for half in (1, 0) for d in fl["ds"] for o in order if half == 1 or (o, d) not in first]
    lag = fl["lag"]
    done = [0]
    def advance(k):
        while done[0] < min(k, len(units)):
            if fl["xy"]: xysend(*units[done[0]])
            done[0] += 1
    def relays(d):
        @pl.when(t == 0)
        def _():
            for o in (1, 2):
                if not via_odd(o, d):
                    landed(1, o, d)
                    relay(d, o, 1, 2)
        @pl.when(t == 1)
        def _():
            for o in (2, 3):
                if via_odd(o, d):
                    landed(2, o, d)
                    relay(d, o, 2, 1)
    for n, u in enumerate(units):
        advance(n + 1 + lag)
        if n == fl["at"]:
            for k in first[up:]:
                far_send(*k)
        half, o, d = u
        if half == 0 and units[n - 1][2] != d or n == 16 and fl["relay"]:
            if n == 16:
                for k in first:
                    far_pass(*k)
            relays(d)
        if o > 0:
            zsend(half, o, d)
        elif half == 1:
            if fl["xy"]: arrived(g.at[1, b, eight(d)], rxy.at[0, 1, yg(d)])
            if fl["relay"]:
                @pl.when(t == 0)
                def _():
                    relay(d, 0, 1, 2)

    def settle(h, d):
        for k in range(2):
            for p in range(2):
                x = g[h, :, pl.ds(yg(d) * 8 + 4 * k, 4), p].reshape(256, 128)
                r = jnp.dot(pm[...], x, preferred_element_type=jnp.float32)
                r = r.astype(jnp.bfloat16).reshape(8, 32, 128)
                ys[h, :, p, pl.ds(pl.multiple_of(yg(d) * 64 + 32 * k, 32), 32), :] = r

    @pl.when(t == 1)
    def _():
        for d in range(4):
            for o in (2, 3, 1):
                landed(1, o, d)
            settle(1, d)

    for d in fl["last"]:
        arrived(g.at[0, b, eight(d)], rxy.at[0, 0, yg(d)])
        for o in (2, 3, 1):
            landed(0, o, d)
        settle(0, d)
    for d in range(4):
        @pl.when(t == 0)
        def _():
            for o in (2, 3):
                if via_odd(o, d):
                    landed(1, o, d)

        @pl.when(t == 1)
        def _():
            for o in (0, 1, 2):
                if not via_odd(o, d):
                    landed(2, o, d)
        settle(1 + t, d)
    for o in range(4):
        for half in range(2):
            gone = [d for (oo, d) in first if oo == o] if half == 0 else []
            if fl["xy"]: arrived(s.at[0, 0, pl.ds(0, 31 - 8 * len(gone))], sx.at[o, half])
            if o > 0:
                arrived(s.at[0, 0, pl.ds(0, 32 - 8 * len(gone))], sz.at[o, half])
    if fl['relay']:
        for o in range(4):
            for d in range(4):
                @pl.when(t == (1 if via_odd(o, d) else 0))
                def _():
                    arrived(s.at[0, 0, pl.ds(0, 8)], sr.at[o, d])
    for k in range(len(first)):
        arrived(s1.at[k], sf.at[k])
        arrived(s1.at[k], sg.at[k])


def comm(v, pm):
    bf = jnp.bfloat16
    D = pltpu.SemaphoreType.DMA
    return pl.pallas_call(
        functools.partial(comm_kernel, dict(FL)),
        out_shape=pltpu.VMEM((3, 8, 2, 256, 128), bf),
        in_specs=[pl.BlockSpec(memory_space=pl.ANY), pl.BlockSpec(memory_space=pltpu.VMEM)],
        out_specs=pl.BlockSpec(memory_space=pltpu.VMEM),
        scratch_shapes=[
            pltpu.VMEM((3, 2, 32, 2, 2, 8, 128), bf),
            pltpu.VMEM((3, 4, 32, 2, 2, 8, 128), bf),
            pltpu.VMEM((max(1, len(FL["first"])), 2, 2, 8, 8, 128), bf),
            D((4, 2, 4)), D((3, 4, 4)), D((4, 2)), D((4, 2)), D((4, 4)), D((12,)), D((12,)), D((12,)),
        ],
        compiler_params=pltpu.CompilerParams(collective_id=0, has_side_effects=True),
        name="gather",
    )(v.reshape(2, 2, 32, 4, 8, 256), pm)


def corr_kernel(tap, y_ref, out, o_ref, sem):
    def leave(n):
        return pltpu.make_async_copy(o_ref.at[:, n], out.at[:, n], sem.at[n])

    for n in range(8):
        one(tap, y_ref, o_ref, n)
        leave(n).start()
    for n in range(8):
        leave(n).wait()


def one(tap, y_ref, o_ref, n):
    ch = n
    early, late = tap[0:1, :], tap[1:2, :]
    t = lax.axis_index("tm")
    f32, bf = jnp.float32, jnp.bfloat16

    def load(h, p):
        return y_ref[h, ch, p].astype(f32)

    def window(w, lo, ea):
        al, bl_, ae, be = lo[0], lo[1], ea[0], ea[1]
        rhs = jnp.concatenate([al, bl_, ae, be], 1)
        lhs = jnp.concatenate([bl_, -al, be, -ae], 1)
        for i, m in enumerate((rhs, lhs)):
            r = lax.dot_general(m, rhs, (((1,), (1,)), ((), ())), preferred_element_type=f32)
            o_ref[i, n, w] = (r * (1.0 / 128)).astype(bf)

    a = [load(0, p) for p in (0, 1)]
    tail = [(load(2, p) * early) for p in (0, 1)]
    tail = [jnp.where(t == 1, x, 0.0).astype(bf) for x in tail]
    window(0, [(x * late).astype(bf) for x in a], tail)
    bb = [load(1, p) for p in (0, 1)]
    window(1, [(x * late).astype(bf) for x in bb], [(x * early).astype(bf) for x in a])


def corr(tap, y):
    return pl.pallas_call(
        corr_kernel,
        out_shape=jax.ShapeDtypeStruct((2, 8, 2, 256, 256), jnp.bfloat16),
        in_specs=[pl.BlockSpec(memory_space=pltpu.VMEM)] * 2,
        out_specs=pl.BlockSpec(memory_space=pl.ANY),
        scratch_shapes=[
            pltpu.VMEM((2, 8, 2, 256, 256), jnp.bfloat16),
            pltpu.SemaphoreType.DMA((8,)),
        ],
        compiler_params=pltpu.CompilerParams(vmem_limit_bytes=24 * 2**20),
        name="corr",
    )(tap, y)


def tapers():
    steps = np.arange(128, dtype=np.float64)
    return np.stack([np.sin(np.pi * (steps + 0.5) / 256), np.sin(np.pi * (steps + 128.5) / 256)]).astype(np.float32)


def perm():
    m = np.zeros((256, 256), np.float32)
    for b in range(4):
        for c in range(4):
            for s in range(2):
                for h in range(8):
                    m[h * 32 + c * 8 + b * 2 + s, ((b * 4 + c) * 2 + s) * 8 + h] = 1
    return m


def local(voltages):
    y = comm(voltages.reshape(2, 2, 128, 8, 256), perm().astype(jnp.bfloat16))
    return corr(tapers(), y)


def solution(mesh):
    return jax.shard_map(
        local,
        mesh=mesh,
        in_specs=(P(None, ("chan", "bl"), None, "tm"),),
        out_specs=P(None, ("chan", "bl"), "tm", None, None),
        check_vma=False,
    )
```
